32 devices in a mesh: grp: 2 (over core), dp: 16 (over z, y, x).
Axes of the slice: x: 2, y: 2, z: 4, core: 2. Of those that a mesh axis runs over, the one named last changes fastest.
Arguments:
- grad: bfloat16 [2, 32768, 8192], P('grp', None, 'dp'), may hold values from -40 to 40
- residual: bfloat16 [2, 32768, 8192], P('grp', None, 'dp'), may hold values from -4 to 4
- q_prev: float32 [5, 4, 8192], P(None, None, 'dp'), may hold values from -0.0625 to 0.0625
- owner_table: int32 [5], replicated, may hold values from 0 to 15, as said below
Outputs:
- new_residual: bfloat16 [2, 32768, 8192], P('grp', None, 'dp')
- q_new: float32 [5, 4, 8192], P(None, None, 'dp')
- owned: float32 [16, 4, 14336], P('dp')
The draws below stay inside these ranges and needn't reach their ends.
Inputs may be any that keep to these rules, and one draw needn't show every extreme that they name: `owner_table`: the 5 owners are distinct.
All inputs are finite; a program needn't handle non-finite values.
Results may differ from the reference program's by a relative error of at most 0.0055.
Values sent between devices are 32-bit elements; how exact they have to be, the bound alone decides.
A program may use at most 192 MiB of HBM per device.

```python
import jax
import jax.numpy as jnp
from jax import lax

D = 8192
KV = 1024
FF_WIN = 14336
LAYERS = 5
RANK = 4
R_ALL = 32768
CAP = 14336
N_GRP = 2
N_DP = 16


def draw_grad(key, part):
    shared = jax.random.normal(jax.random.fold_in(key, 11), (R_ALL, D), jnp.float32)
    private_part = jax.random.normal(jax.random.fold_in(key, 12), (N_GRP, R_ALL, D), jnp.float32)
    values = 0.3 * shared[None] + 0.95 * private_part
    return jnp.clip(values, -40.0, 40.0).astype(jnp.bfloat16)


def draw_owner_table(key, part):
    middle = jax.random.permutation(jax.random.fold_in(key, 21), N_DP - 2)[:LAYERS - 2].astype(jnp.int32) + 1
    ends = jnp.array([0, N_DP - 1], jnp.int32)
    table = jnp.concatenate([ends, middle])
    order = jax.random.permutation(jax.random.fold_in(key, 22), LAYERS)
    return table[order].astype(jnp.int32)


def steps_of(stream_key, dims, cuts, least, high):
    gain, own = 1.0, jax.random.fold_in(stream_key, 6)
    for axis_at, shards_of in cuts:
        draws = jnp.exp(jax.random.uniform(jax.random.fold_in(own, axis_at), (shards_of,), jnp.float32, least / len(cuts), high / len(cuts)))
        gain = gain * jnp.repeat(draws, dims[axis_at] // shards_of).reshape([-1 if axis == axis_at else 1 for axis in range(len(dims))])
    return gain


def bell_draw(key, shape, scale, limit, cuts=(), kind=jnp.bfloat16):
    drawn = jax.random.normal(key, shape, jnp.float32) * scale
    if len(cuts) > 0:
        drawn = steps_of(key, shape, cuts, -0.22, 0.18) * drawn
    return jnp.clip(drawn, min=-limit, max=limit).astype(kind)


def setup_inputs(seed: int = 0) -> dict:
    streams_of = jax.random.split(jax.random.key(seed), 5)
    grad = draw_grad(jax.random.fold_in(streams_of[4], 71), 0)
    residual = bell_draw(streams_of[1], (N_GRP, R_ALL, D), 0.5, 4.0, ((0, 2), (2, 16)))
    q_prev = bell_draw(streams_of[2], (LAYERS, RANK, D), D ** -0.5, 0.0625, ((2, 16),), jnp.float32)
    owner_table = draw_owner_table(jax.random.fold_in(streams_of[4], 71), 0)
    return {"grad": grad, "residual": residual, "q_prev": q_prev, "owner_table": owner_table}


EPSILON = 1e-06

def block_sizes():
    return [D, KV, KV, D, FF_WIN]

def whiten(lower_factor, projected):
    solved = []
    for i in range(projected.shape[-2]):
        running = projected[..., i, :]
        for k in range(i):
            running = running - lower_factor[..., i, k, None] * solved[k]
        solved.append(running / lower_factor[..., i, i, None])
    return jnp.stack(solved, axis=-2)

def orthonormal(projected):
    gram_matrix = jnp.dot(projected, projected.T, precision=lax.Precision.HIGHEST)
    gram_matrix = gram_matrix + EPSILON * jnp.eye(projected.shape[0], dtype=jnp.float32)
    return whiten(jnp.linalg.cholesky(gram_matrix), projected)

def reference(grad, residual, q_prev, owner_table):
    owned = jnp.zeros((N_DP, RANK, CAP), jnp.float32)
    residuals = []
    q_list = []
    offset = 0
    for layer_id, count in enumerate(block_sizes()):
        compensated = (grad[:, offset:offset + count].astype(jnp.float32) + residual[:, offset:offset + count].astype(jnp.float32)).astype(jnp.bfloat16)
        q_rounded = q_prev[layer_id].astype(jnp.bfloat16)
        projected = jnp.zeros((RANK, count), jnp.float32)
        for group in range(N_GRP):
            projected = projected + lax.dot_general(q_rounded.astype(jnp.float32), compensated[group].astype(jnp.float32), (((1,), (1,)), ((), ())), preferred_element_type=jnp.float32)
        projected = projected / N_GRP
        padded = jnp.pad(projected, ((0, 0), (0, CAP - count)))
        owned = lax.dynamic_update_slice(owned, padded[None], (owner_table[layer_id], jnp.int32(0), jnp.int32(0)))
        basis_rounded = orthonormal(projected).astype(jnp.bfloat16)
        q_sum = jnp.zeros((RANK, D), jnp.float32)
        for group in range(N_GRP):
            q_sum = q_sum + jnp.dot(basis_rounded.astype(jnp.float32), compensated[group].astype(jnp.float32), preferred_element_type=jnp.float32)
        q_new = q_sum / N_GRP
        q_round = q_new.astype(jnp.bfloat16)
        update = lax.dot_general(basis_rounded.astype(jnp.float32), q_round.astype(jnp.float32), (((0,), (0,)), ((), ())), preferred_element_type=jnp.float32)
        residuals.append((compensated.astype(jnp.float32) - update[None]).astype(jnp.bfloat16))
        q_list.append(q_new)
        offset += count
    return (jnp.concatenate(residuals, axis=1), jnp.stack(q_list), owned)
```

```python
import functools

import jax
import jax.numpy as jnp
from jax import lax
from jax.experimental import pallas as pl
from jax.experimental.pallas import tpu as pltpu
from jax.sharding import PartitionSpec as P

D = 8192
KV = 1024
FF_WIN = 14336

EPSILON = 1e-06
CHUNK = 1024
SUB = 256
DOT_ROWS = 4096
SOLVE_LANES = 1024
UPDATE_ROWS = 2048
SLOTS = 8
OUT_SLOTS = 6
MESH = pl.DeviceIdType.MESH
STAGES = ((4,), (3,), (0,), (1, 2))
EARLY_LAYER, EARLY_ROWS = 4, 8192


def block_sizes():
    return [D, KV, KV, D, FF_WIN]


def block_offsets():
    offsets, at = [], 0
    for count in block_sizes():
        offsets.append(at)
        at += count
    return offsets


def piece_lanes(stage, peers):
    count = sum(block_sizes()[layer] for layer in stage)
    return -(-count // (2 * peers * 128)) * 128


def even_split(count, most):
    parts = -(-count // most)
    while count % (parts * 128):
        parts += 1
    return count // parts


def updated_rows(basis, q_round, comp):
    update = lax.dot_general(basis, q_round, (((0,), (0,)), ((), ())), preferred_element_type=jnp.float32)
    return (comp.astype(jnp.float32) - update).astype(jnp.bfloat16)


def gather_kernel(peers, groups, grad_ref, res_ref, q_hbm, *refs):
    sizes, offsets = block_sizes(), block_offsets()
    n_chunks = grad_ref.shape[1] // CHUNK
    n_st, n_layers = len(STAGES), len(sizes)
    comp, (basis_ref, qnew_ref, proj_ref), scratch = refs[:n_layers], refs[n_layers : n_layers + 3], refs[n_layers + 3 :]
    q_ref, ring, qpart, qrecv = scratch[:4]
    bufs = scratch[4 : 4 + 5 * n_st]
    qsem, gsem, rsem, ssem, vsem, qssem, qrsem = scratch[4 + 5 * n_st :]
    part, sib, hs, recv, full = (bufs[i * n_st : (i + 1) * n_st] for i in range(5))
    g, d = lax.axis_index("grp"), lax.axis_index("dp")
    other = 1 - g
    rank = q_ref.shape[1]
    order = [layer for stage in STAGES for layer in stage]
    first_of, at = {}, 0
    for layer in order:
        first_of[layer] = at
        at += sizes[layer] // CHUNK

    def loads(i, layer):
        slot = lax.rem(i, SLOTS)
        local = pl.multiple_of((i - first_of[layer]) * CHUNK, CHUNK)
        at = pl.multiple_of(local + offsets[layer], CHUNK)
        return (
            pltpu.make_async_copy(grad_ref.at[0, pl.ds(at, CHUNK)], comp[layer].at[pl.ds(local, CHUNK)], gsem.at[slot]),
            pltpu.make_async_copy(res_ref.at[0, pl.ds(at, CHUNK)], ring.at[slot], rsem.at[slot]),
        )

    def spans(first, last):
        for layer in order:
            lo = max(first, first_of[layer])
            hi = min(last, first_of[layer] + sizes[layer] // CHUNK)
            if lo < hi:
                yield layer, lo, hi

    q_load = pltpu.make_async_copy(q_hbm, q_ref, qsem)
    q_load.start()
    for ahead, lo, hi in spans(0, SLOTS):

        @pl.loop(lo, hi)
        def _(i):
            for copy in loads(i, ahead):
                copy.start()

    barrier = pltpu.get_barrier_semaphore()
    pl.semaphore_signal(barrier, inc=1, device_id=(other, d), device_id_type=MESH)

    @pl.loop(1, peers)
    def _(j):
        pl.semaphore_signal(barrier, inc=1, device_id=(g, lax.rem(d + j, peers)), device_id_type=MESH)

    for s, stage in enumerate(STAGES):
        used = sum(sizes[layer] for layer in stage)
        if used < part[s].shape[1]:
            part[s][:, used:] = jnp.zeros((rank, part[s].shape[1] - used), jnp.float32)

    q_load.wait()

    def stream(first, last, s, base, layer):
        qb = q_ref[layer].astype(jnp.bfloat16)
        col0 = base - first_of[layer] * CHUNK

        def step(i, ahead):
            for copy in loads(i, layer):
                copy.wait()
            slot = lax.rem(i, SLOTS)
            at = pl.multiple_of((i - first_of[layer]) * CHUNK, CHUNK)
            col = pl.multiple_of(col0 + i * CHUNK, CHUNK)
            for u in range(0, CHUNK, SUB):
                rng = pl.ds(at + u, SUB)
                total = comp[layer][rng, :] + ring[slot, u : u + SUB, :]
                comp[layer][rng, :] = total
                part[s][:, pl.ds(col + u, SUB)] = lax.dot_general(
                    qb, total, (((1,), (1,)), ((), ())), preferred_element_type=jnp.float32
                )
            if ahead is not None:
                for copy in loads(i + SLOTS, ahead):
                    copy.start()

        for ahead, lo, hi in spans(first + SLOTS, last + SLOTS):
            pl.loop(lo - SLOTS, hi - SLOTS)(functools.partial(step, ahead=ahead))
        alone = max(first, n_chunks - SLOTS)
        if alone < last:
            pl.loop(alone, last)(functools.partial(step, ahead=None))

    def to_sibling(src, dst, s, phase):
        return pltpu.make_async_remote_copy(
            src_ref=src, dst_ref=dst, send_sem=ssem.at[s, phase], recv_sem=vsem.at[s, phase],
            device_id=(other, d), device_id_type=MESH,
        )

    def half_copy(s):
        width = sib[s].shape[1]
        src = part[s].at[:, pl.ds(pl.multiple_of(other * width, 128), width)]
        return to_sibling(src, sib[s], s, 0)

    def f0(s):
        half_copy(s).start()

    def scatter(s, j):
        to, width = lax.rem(d + j, peers), recv[s].shape[2]
        return pltpu.make_async_remote_copy(
            src_ref=hs[s].at[:, pl.ds(pl.multiple_of(to * width, 128), width)], dst_ref=recv[s].at[d],
            send_sem=ssem.at[s, 1], recv_sem=vsem.at[s, 1], device_id=(g, to), device_id_type=MESH,
        )

    def f1(s):
        half_copy(s).wait_recv()
        width, piece = sib[s].shape[1], recv[s].shape[2]
        hs[s][...] = part[s][:, pl.ds(pl.multiple_of(g * width, 128), width)] + sib[s][...]
        recv[s][d] = hs[s][:, pl.ds(pl.multiple_of(d * piece, 128), piece)]

        @pl.loop(1, peers)
        def _(j):
            scatter(s, j).start()

    def all_of(s, sem):
        ref = recv[s].at[pl.ds(0, peers - 1)]
        return pltpu.make_async_copy(ref, ref, sem)

    def my_cols(s):
        piece = recv[s].shape[2]
        return pl.ds(pl.multiple_of((g * peers + d) * piece, 128), piece)

    def f2(s):
        all_of(s, vsem.at[s, 1]).wait()
        full[s][:, my_cols(s)] = jnp.sum(recv[s][...], axis=0) / groups

        @pl.loop(1, peers)
        def _(j):
            mine = full[s].at[:, my_cols(s)]
            pltpu.make_async_remote_copy(
                src_ref=mine, dst_ref=mine, send_sem=ssem.at[s, 2], recv_sem=vsem.at[s, 2],
                device_id=(g, lax.rem(d + j, peers)), device_id_type=MESH,
            ).start()

    def full_copy(s):
        width = sib[s].shape[1]
        half = full[s].at[:, pl.ds(pl.multiple_of(g * width, 128), width)]
        return to_sibling(half, half, s, 3)

    def f3(s):
        all_of(s, vsem.at[s, 2]).wait()
        full_copy(s).start()

    def q_copy(layer):
        return pltpu.make_async_remote_copy(
            src_ref=qpart.at[layer], dst_ref=qrecv.at[layer], send_sem=qssem.at[layer], recv_sem=qrsem.at[layer],
            device_id=(other, d), device_id_type=MESH,
        )

    def solve(s, base, layer):
        count, off = sizes[layer], offsets[layer]
        lanes = min(SOLVE_LANES, count)

        def gram(i, sums):
            sums = list(sums)
            for v in range(0, lanes, 128):
                cols = pl.ds(pl.multiple_of(base + i * lanes + v, 128), 128)
                block = full[s][:, cols]
                proj_ref[:, pl.ds(pl.multiple_of(off + i * lanes + v, 128), 128)] = block
                for k in range(rank):
                    sums[k] = sums[k] + block * full[s][k : k + 1, cols]
            return tuple(sums)

        sums = lax.fori_loop(0, count // lanes, gram, tuple(jnp.zeros((rank, 128), jnp.float32) for _ in range(rank)))
        row_id = lax.broadcasted_iota(jnp.int32, (rank, 1), 0)
        cols = [
            jnp.sum(acc, axis=1, keepdims=True) + jnp.where(row_id == k, EPSILON, 0.0) for k, acc in enumerate(sums)
        ]
        lane_id = lax.broadcasted_iota(jnp.int32, (rank, 128), 1)
        inverse = jnp.where(lane_id == lax.broadcasted_iota(jnp.int32, (rank, 128), 0), 1.0, 0.0).astype(jnp.float32)
        for k in range(rank):
            scale = 1.0 / jnp.sqrt(cols[k][k : k + 1, :])
            low = cols[k] * scale
            for j in range(k + 1, rank):
                cols[j] = cols[j] - low * low[j : j + 1, :]
            row = inverse[k : k + 1, :] * scale
            below = jnp.where(row_id > k, low, 0.0)
            inverse = jnp.where(row_id == k, row, inverse - below * row)
        weights = [inverse[:, k : k + 1] for k in range(rank)]

        @pl.loop(0, count // lanes)
        def _(i):
            cols = pl.ds(pl.multiple_of(base + i * lanes, 128), lanes)
            total = weights[0] * full[s][0:1, cols]
            for k in range(1, rank):
                total = total + weights[k] * full[s][k : k + 1, cols]
            basis_ref[:, pl.ds(pl.multiple_of(off + i * lanes, 128), lanes)] = total.astype(jnp.bfloat16)

        rows = even_split(count, DOT_ROWS)

        def dot(i, acc):
            here = pl.multiple_of(i * rows, rows)
            return acc + jnp.dot(
                basis_ref[:, pl.ds(pl.multiple_of(off + here, 128), rows)], comp[layer][pl.ds(here, rows), :],
                preferred_element_type=jnp.float32,
            )

        qpart[layer] = lax.fori_loop(0, count // rows, dot, jnp.zeros(qpart.shape[1:], jnp.float32))
        q_copy(layer).start()

    def f4(s):
        full_copy(s).wait_recv()
        base = 0
        for layer in STAGES[s]:
            solve(s, base, layer)
            base += sizes[layer]

    def f5(layer):
        q_copy(layer).wait()
        qnew_ref[layer] = (qpart[layer] + qrecv[layer]) / groups

    def f6(layer, first, last):
        q_round = qnew_ref[layer].astype(jnp.bfloat16)

        @pl.loop(first, last)
        def _(i):
            at = pl.multiple_of(i * UPDATE_ROWS, UPDATE_ROWS)
            for u in range(0, UPDATE_ROWS, SUB):
                cols = pl.ds(pl.multiple_of(offsets[layer] + at + u, 128), SUB)
                rng = pl.ds(at + u, SUB)
                comp[layer][rng, :] = updated_rows(basis_ref[:, cols], q_round, comp[layer][rng, :])

    def part_of(layer, lo, hi):
        s = [k for k, stage in enumerate(STAGES) if layer in stage][0]
        base = 0
        for before in STAGES[s]:
            if before == layer:
                break
            base += sizes[before]
        stream(first_of[layer] + lo, first_of[layer] + hi, s, base, layer)

    n = [sizes[layer] // CHUNK for layer in range(len(sizes))]

    def scoped(name, fn, *args):
        with jax.named_scope(name):
            fn(*args)

    scoped("s4", part_of, 4, 0, n[4])
    pl.semaphore_wait(barrier, peers)
    scoped("f0_0", f0, 0)
    scoped("s3a", part_of, 3, 0, 2)
    scoped("f1_0", f1, 0)
    scoped("s3b", part_of, 3, 2, n[3])
    scoped("f0_1", f0, 1)
    scoped("s0a", part_of, 0, 0, 2)
    scoped("f1_1", f1, 1)
    scoped("s0b", part_of, 0, 2, 5)
    scoped("f2_0", f2, 0)
    scoped("s0c", part_of, 0, 5, n[0])
    scoped("f0_2", f0, 2)
    scoped("s1", part_of, 1, 0, n[1])
    scoped("s2", part_of, 2, 0, n[2])
    scoped("f0_3", f0, 3)
    scoped("f1_2", f1, 2)
    scoped("f2_1", f2, 1)
    scoped("f3_0", f3, 0)
    scoped("f1_3", f1, 3)
    scoped("f4_0", f4, 0)
    scoped("f2_2", f2, 2)
    scoped("f3_1", f3, 1)
    scoped("f2_3", f2, 3)
    scoped("f5_4", f5, 4)
    scoped("f4_1", f4, 1)
    scoped("f6a", f6, 4, 0, 2)
    scoped("f3_2", f3, 2)
    scoped("f6b", f6, 4, 2, 3)
    scoped("f3_3", f3, 3)
    scoped("f4_2", f4, 2)
    scoped("f4_3", f4, 3)
    scoped("f6c", f6, 4, 3, EARLY_ROWS // UPDATE_ROWS)
    scoped("f5_3", f5, 3)
    scoped("f5_0", f5, 0)
    scoped("f5_1", f5, 1)
    scoped("f5_2", f5, 2)
    for s in range(n_st):
        half_copy(s).wait_send()
        all_of(s, ssem.at[s, 1]).wait()
        all_of(s, ssem.at[s, 2]).wait()
        full_copy(s).wait_send()


def write_kernel(tbl_hbm, basis_ref, q_ref, proj_ref, *refs):
    sizes, offsets = block_sizes(), block_offsets()
    n_layers = len(sizes)
    comp, (out_ref, qout_ref, owned_ref), scratch = refs[:n_layers], refs[n_layers : n_layers + 3], refs[n_layers + 3 :]
    ring, mine, table, sem, esem, tsem, qsem, osem = scratch
    tbl_copy = pltpu.make_async_copy(tbl_hbm, table, tsem)
    tbl_copy.start()

    ready = pltpu.make_async_copy(
        comp[EARLY_LAYER].at[pl.ds(0, EARLY_ROWS)], out_ref.at[0, pl.ds(offsets[EARLY_LAYER], EARLY_ROWS)], esem
    )
    ready.start()
    q_copy = pltpu.make_async_copy(q_ref, qout_ref, qsem)
    q_copy.start()

    def store(i, at):
        slot = lax.rem(i, OUT_SLOTS)
        return pltpu.make_async_copy(
            ring.at[slot], out_ref.at[0, pl.ds(pl.multiple_of(at, CHUNK), UPDATE_ROWS)], sem.at[slot]
        )

    def fill(slot, into, layer, at, rows):
        q_round = q_ref[layer].astype(jnp.bfloat16)
        for u in range(0, rows, SUB):
            cols = pl.ds(pl.multiple_of(offsets[layer] + at + u, 128), SUB)
            ring[slot, into + u : into + u + SUB, :] = updated_rows(
                basis_ref[:, cols], q_round, comp[layer][pl.ds(at + u, SUB), :]
            )

    done = 0
    for layer in (3, 0, 4):
        first = EARLY_ROWS if layer == EARLY_LAYER else 0

        @pl.loop(0, (sizes[layer] - first) // UPDATE_ROWS)
        def _(j):
            i = done + j
            at = pl.multiple_of(first + j * UPDATE_ROWS, UPDATE_ROWS)

            @pl.when(i >= OUT_SLOTS)
            def _():
                store(i, 0).wait()

            fill(lax.rem(i, OUT_SLOTS), 0, layer, at, UPDATE_ROWS)
            store(i, offsets[layer] + at).start()

        done += (sizes[layer] - first) // UPDATE_ROWS
    store(done, 0).wait()
    fill(done % OUT_SLOTS, 0, 1, 0, sizes[1])
    fill(done % OUT_SLOTS, sizes[1], 2, 0, sizes[2])
    store(done, offsets[1]).start()
    done += 1

    mine[...] = jnp.zeros_like(mine)
    tbl_copy.wait()
    me = lax.axis_index("dp")
    for layer, count in enumerate(sizes):

        @pl.when(table[layer] == me)
        def _():
            mine[0, :, :count] = proj_ref[:, offsets[layer] : offsets[layer] + count]

    own_copy = pltpu.make_async_copy(mine, owned_ref, osem)
    own_copy.start()

    @pl.loop(max(0, done - OUT_SLOTS), done)
    def _(i):
        store(i, 0).wait()

    ready.wait()
    q_copy.wait()
    own_copy.wait()


def body(peers, groups, grad, residual, q_prev, owner_table):
    _, rows, cols = grad.shape
    layers, rank, _ = q_prev.shape
    cap = max(block_sizes())
    n_st = len(STAGES)
    piece = [piece_lanes(stage, peers) for stage in STAGES]
    f32 = jnp.float32
    vmem = pl.BlockSpec(memory_space=pltpu.VMEM)
    hbm = pl.BlockSpec(memory_space=pltpu.HBM)
    *comp, basis, q_new, proj = pl.pallas_call(
        functools.partial(gather_kernel, peers, groups),
        out_shape=(
            *[pltpu.VMEM((count, cols), jnp.bfloat16) for count in block_sizes()],
            pltpu.VMEM((rank, rows), jnp.bfloat16),
            pltpu.VMEM((layers, rank, cols), f32),
            pltpu.VMEM((rank, rows), f32),
        ),
        in_specs=[hbm, hbm, hbm],
        out_specs=(vmem,) * (layers + 3),
        scratch_shapes=[
            pltpu.VMEM((layers, rank, cols), f32),
            pltpu.VMEM((SLOTS, CHUNK, cols), jnp.bfloat16),
            pltpu.VMEM((layers, rank, cols), f32),
            pltpu.VMEM((layers, rank, cols), f32),
        ]
        + [pltpu.VMEM((rank, 2 * peers * p), f32) for p in piece]
        + [pltpu.VMEM((rank, peers * p), f32) for p in piece]
        + [pltpu.VMEM((rank, peers * p), f32) for p in piece]
        + [pltpu.VMEM((peers, rank, p), f32) for p in piece]
        + [pltpu.VMEM((rank, 2 * peers * p), f32) for p in piece]
        + [
            pltpu.SemaphoreType.DMA,
            pltpu.SemaphoreType.DMA((SLOTS,)),
            pltpu.SemaphoreType.DMA((SLOTS,)),
            pltpu.SemaphoreType.DMA((n_st, 4)),
            pltpu.SemaphoreType.DMA((n_st, 4)),
            pltpu.SemaphoreType.DMA((layers,)),
            pltpu.SemaphoreType.DMA((layers,)),
        ],
        compiler_params=pltpu.CompilerParams(
            collective_id=0, has_side_effects=True, vmem_limit_bytes=14 * 1024 * 1024
        ),
        name="stream_and_project",
    )(grad, residual, q_prev)
    new_residual, q_out, owned = pl.pallas_call(
        write_kernel,
        out_shape=(
            jax.ShapeDtypeStruct((1, rows, cols), jnp.bfloat16),
            jax.ShapeDtypeStruct((layers, rank, cols), f32),
            jax.ShapeDtypeStruct((1, rank, cap), f32),
        ),
        in_specs=[hbm] + [vmem] * (layers + 3),
        out_specs=(hbm, hbm, hbm),
        scratch_shapes=[
            pltpu.VMEM((OUT_SLOTS, UPDATE_ROWS, cols), jnp.bfloat16),
            pltpu.VMEM((1, rank, cap), f32),
            pltpu.SMEM((layers,), jnp.int32),
            pltpu.SemaphoreType.DMA((OUT_SLOTS,)),
            pltpu.SemaphoreType.DMA,
            pltpu.SemaphoreType.DMA,
            pltpu.SemaphoreType.DMA,
            pltpu.SemaphoreType.DMA,
        ],
        compiler_params=pltpu.CompilerParams(vmem_limit_bytes=16 * 1024 * 1024),
        name="write_residual",
    )(owner_table, basis, q_new, proj, *comp)
    return new_residual, q_out, owned


def solution(mesh):
    in_specs = (P("grp", None, "dp"), P("grp", None, "dp"), P(None, None, "dp"), P())
    out_specs = (P("grp", None, "dp"), P(None, None, "dp"), P("dp", None, None))
    fn = functools.partial(body, mesh.shape["dp"], mesh.shape["grp"])
    return jax.shard_map(fn, mesh=mesh, in_specs=in_specs, out_specs=out_specs, check_vma=False)
```
